32 devices in a mesh: dp: 4 (over x, core), tensor: 8 (over z, y).
Axes of the slice: x: 2, y: 2, z: 4, core: 2. Of those that a mesh axis runs over, the one named last changes fastest.
Arguments:
- attn_ctx: bfloat16 [2048, 8192], P('dp', 'tensor'), may hold values from -6 to 6
- w_out: bfloat16 [8192, 8192], P('tensor'), may hold values from -0.09375 to 0.09375
- resid: bfloat16 [2048, 8192], P(('dp', 'tensor')), may hold values from -6 to 6
- teacher_gain: bfloat16 [8192], replicated, may hold values from 0.25 to 1.75
- dest_row: int32 [2048], replicated, may hold values from 0 to 2047, as said below
- student_in: bfloat16 [2048, 4096], P('dp', 'tensor'), may hold values from -6 to 6
- student_gain: bfloat16 [4096], replicated, may hold values from 0.25 to 1.75
- w_gate: bfloat16 [4096, 14336], P('dp', 'tensor'), may hold values from -0.09375 to 0.09375
- w_up: bfloat16 [4096, 14336], P('dp', 'tensor'), may hold values from -0.09375 to 0.09375
- w_down: bfloat16 [14336, 4096], P('tensor', 'dp'), may hold values from -0.0625 to 0.0625
- proj: bfloat16 [4096, 8192], P('dp', 'tensor'), may hold values from -0.09375 to 0.09375
Outputs:
- student_out: bfloat16 [2048, 4096], P('dp', 'tensor')
- row_loss: float32 [2048], P('dp')
- residue: float32 [2048, 8192], P('dp', 'tensor')
The draws below stay inside these ranges and needn't reach their ends.
Inputs may be any that keep to these rules, and one draw needn't show every extreme that they name: A permutation of the rows; of the 64 rows i in one aligned block of teacher rows, at most 32 have dest_row[i] in any one tile of 512 student rows, and some tile receives exactly 32 of them.
All inputs are finite; a program needn't handle non-finite values.
Results may differ from the reference program's by a relative error of at most 0.012.
Values may be sent and summed in bfloat16 or wider, within the bound.
A program may use at most 192 MiB of HBM per device.

```python
import jax
import jax.numpy as jnp
from jax import lax

HT = 8192
D = 4096
FF = 14336
TT = 512
TOKENS = 2048
N_DP = 4
N_TENSOR = 8


def draw_dest_row(key, part):
    rows_dev = TT // N_TENSOR
    mean_count = rows_dev // N_DP
    sources = N_DP * N_TENSOR
    keys = jax.random.split(jax.random.fold_in(key, 7), 5)
    amounts = jax.random.randint(keys[0], (N_DP // 2,), 0, mean_count + 1)
    amounts = amounts.at[0].set(mean_count)
    counts = jnp.stack([mean_count + amounts, mean_count - amounts], 1).reshape(N_DP)
    counts = counts[jax.random.permutation(keys[1], N_DP)]
    rotation = jax.random.permutation(keys[2], sources) % N_DP
    shifted = (jnp.arange(N_DP)[None, :] + rotation[:, None]) % N_DP
    per_source = counts[shifted]
    bounds = jnp.cumsum(per_source, 1)
    position = jnp.arange(rows_dev)
    labels = jnp.sum((position[None, :, None] >= bounds[:, None, :]).astype(jnp.int32), 2)
    orders = jax.vmap(lambda one_key: jax.random.permutation(one_key, rows_dev))(jax.random.split(keys[3], sources))
    labels = jnp.take_along_axis(labels, orders, 1).reshape(-1)
    onehot = (labels[:, None] == jnp.arange(N_DP)[None, :]).astype(jnp.int32)
    ranking = jnp.sum((jnp.cumsum(onehot, 0) - onehot) * onehot, 1)
    placing = jax.vmap(lambda one_key: jax.random.permutation(one_key, TT))(jax.random.split(keys[4], N_DP))
    return (labels * TT + placing[labels, ranking]).astype(jnp.int32)


def with_spikes(drawn, stream_key, source, target, parts, factor):
    def block_of(axis_at):
        return (jnp.arange(drawn.shape[axis_at]) // (drawn.shape[axis_at] // parts)).reshape((-1,) + (1,) * (drawn.ndim - 1 - axis_at))

    near = jax.random.permutation(stream_key, parts)[block_of(target)]
    far = (block_of(target) + parts // 2) % parts
    return jnp.where((block_of(source) == near) | (block_of(source) == far), factor * drawn, drawn)


def level_of(stream_key, shape, cuts, least, high):
    factor_of = 1.0
    for dim, blocks in cuts:
        heights = jax.random.uniform(jax.random.fold_in(jax.random.fold_in(stream_key, 6), dim), (blocks,), jnp.float32, least / len(cuts), high / len(cuts))
        factor_of = factor_of * jnp.repeat(jnp.exp(heights), shape[dim] // blocks).reshape((-1,) + (1,) * (len(shape) - 1 - dim))
    return factor_of


def scatter_about(own_key, extent, scale, bound, cuts=(), kind=jnp.bfloat16):
    values = jax.random.normal(own_key, extent, jnp.float32) * scale
    if len(cuts) > 0:
        values = level_of(own_key, extent, cuts, -0.22, 0.18) * values
    return jnp.clip(values, min=-bound, max=bound).astype(kind)


def gaussian_with(key, shape, width, bound, cuts, heavy, dtype=jnp.bfloat16):
    values = width * jax.random.normal(key, shape, jnp.float32)
    if cuts:
        values = values * level_of(key, shape, cuts, -0.22, 0.18)
    return jnp.clip(with_spikes(values, jax.random.fold_in(key, 3), *heavy), -bound, bound).astype(dtype)


def setup_inputs(seed: int = 0) -> dict:
    splits = jax.random.split(jax.random.key(seed), 12)
    attn_ctx = scatter_about(splits[0], (TOKENS, HT), 1.0, 6.0, ((0, 4), (1, 8)))
    w_out = gaussian_with(splits[1], (HT, HT), HT ** -0.5, 0.09375, ((0, 8),), (0, 1, 8, 2.0))
    resid = scatter_about(splits[2], (TOKENS, HT), 1.0, 6.0, ((0, 32),))
    teacher_gain = jnp.clip(1.0 + 0.15 * jax.random.normal(splits[3], (HT,), jnp.float32), 0.25, 1.75).astype(jnp.bfloat16)
    dest_row = draw_dest_row(jax.random.fold_in(splits[11], 71), 0)
    student_in = scatter_about(splits[5], (TOKENS, D), 1.0, 6.0, ((0, 4), (1, 8)))
    student_gain = jnp.clip(1.0 + 0.15 * jax.random.normal(splits[6], (D,), jnp.float32), 0.25, 1.75).astype(jnp.bfloat16)
    w_gate = scatter_about(splits[7], (D, FF), D ** -0.5, 0.09375, ((0, 4), (1, 8)))
    w_up = scatter_about(splits[8], (D, FF), D ** -0.5, 0.09375, ((0, 4), (1, 8)))
    w_down = gaussian_with(splits[9], (FF, D), FF ** -0.5, 0.0625, ((0, 8), (1, 4)), (0, 1, 8, 2.0))
    proj = scatter_about(splits[10], (D, HT), D ** -0.5, 0.09375, ((0, 4), (1, 8)))
    return dict(attn_ctx=attn_ctx, w_out=w_out, resid=resid, teacher_gain=teacher_gain, dest_row=dest_row, student_in=student_in, student_gain=student_gain, w_gate=w_gate, w_up=w_up, w_down=w_down, proj=proj)


def reference(attn_ctx, w_out, resid, teacher_gain, dest_row, student_in, student_gain, w_gate, w_up, w_down, proj):
    blocks_ctx = attn_ctx.reshape(TOKENS, N_TENSOR, HT // N_TENSOR).transpose(1, 0, 2)
    blocks_out = w_out.reshape(N_TENSOR, HT // N_TENSOR, HT)

    def add_term(running, pair):
        term = jnp.dot(pair[0], pair[1], preferred_element_type=jnp.float32)
        term = lax.optimization_barrier(term.astype(jnp.bfloat16)).astype(jnp.float32)
        return (running + term, None)
    attn_sum, unused = lax.scan(add_term, jnp.zeros((TOKENS, HT), jnp.float32), (blocks_ctx, blocks_out))
    teacher_hidden = resid.astype(jnp.float32) + attn_sum
    square_mean = lax.optimization_barrier(jnp.mean(teacher_hidden * teacher_hidden, axis=1, keepdims=True))
    teacher_final = (teacher_hidden * lax.rsqrt(square_mean + 1e-06) * teacher_gain.astype(jnp.float32)).astype(jnp.bfloat16)
    target = jnp.zeros((TOKENS, HT), jnp.bfloat16).at[dest_row].set(teacher_final)
    x_full = student_in.astype(jnp.float32)
    student_mean = lax.optimization_barrier(jnp.mean(x_full * x_full, axis=1, keepdims=True))
    normed = (x_full * lax.rsqrt(student_mean + 1e-05) * student_gain.astype(jnp.float32)).astype(jnp.bfloat16)
    gate_acts = jnp.dot(normed, w_gate, preferred_element_type=jnp.float32)
    up_acts = jnp.dot(normed, w_up, preferred_element_type=jnp.float32)
    hidden = (jax.nn.silu(gate_acts) * up_acts).astype(jnp.bfloat16)
    mlp_sum = jnp.dot(hidden, w_down, preferred_element_type=jnp.float32)
    student_out = (x_full + mlp_sum).astype(jnp.bfloat16)
    pred = jnp.dot(student_out, proj, preferred_element_type=jnp.float32)
    residue = pred - target.astype(jnp.float32)
    row_loss = lax.optimization_barrier(jnp.mean(residue * residue, axis=1))
    return (student_out, row_loss, residue)
```

```python
import jax
import jax.numpy as jnp
from jax import lax
from jax.sharding import PartitionSpec as P


F32 = jnp.float32
BF16 = jnp.bfloat16


def local(
    attn_ctx,
    w_out,
    resid,
    teacher_gain,
    dest_row,
    student_in,
    student_gain,
    w_gate,
    w_up,
    w_down,
    proj,
):
    cores = 2
    n_dp = lax.axis_size("dp")
    n_tensor = lax.axis_size("tensor")
    n_x = n_dp // cores
    dp_at = lax.axis_index("dp")
    tensor_at = lax.axis_index("tensor")
    x_at = dp_at // cores
    core_at = dp_at % cores
    steps = [(s, f) for s in range(n_x) for f in range(cores)]

    def x_move(arr, s):
        pairs = [(((x + s) % n_x) * cores + c, x * cores + c) for x in range(n_x) for c in range(cores)]
        return lax.ppermute(arr, "dp", pairs)

    def core_move(arr):
        pairs = [(x * cores + c, x * cores + 1 - c) for x in range(n_x) for c in range(cores)]
        return lax.ppermute(arr, "dp", pairs)

    def blocks_of(arr):
        found = []
        for s in range(n_x):
            same = arr if s == 0 else x_move(arr, s)
            found += [same, core_move(same)]
        return found

    owners = [((x_at + s) % n_x) * cores + (core_at + f) % cores for s, f in steps]

    gates = blocks_of(w_gate)
    ups = blocks_of(w_up)
    downs = blocks_of(w_down)
    projs = blocks_of(proj)

    x_bf = lax.all_gather(student_in, "tensor", axis=1, tiled=True)

    tile_rows = attn_ctx.shape[0]
    own_rows = resid.shape[0]
    term = jnp.dot(attn_ctx, w_out, preferred_element_type=F32)
    wide = jnp.arange(tile_rows)[:, None] // own_rows == tensor_at
    term = term + jnp.where(wide, jnp.tile(resid, (n_tensor, 1)).astype(F32), 0.0)
    hidden_t = lax.psum_scatter(
        term.astype(BF16), "tensor", scatter_dimension=1, tiled=True
    ).astype(F32)
    ht = w_out.shape[1]
    col_width = ht // n_tensor
    squares = lax.psum(jnp.sum(hidden_t * hidden_t, axis=1), "tensor")
    gain_t = lax.dynamic_slice_in_dim(teacher_gain, tensor_at * col_width, col_width, 0)
    teacher_final = (
        hidden_t * lax.rsqrt(squares / ht + 1e-06)[:, None] * gain_t.astype(F32)[None, :]
    ).astype(BF16)
    finals = blocks_of(teacher_final)

    x_full = x_bf.astype(F32)
    student_mean = jnp.mean(x_full * x_full, axis=1, keepdims=True)
    normed = (x_full * lax.rsqrt(student_mean + 1e-05) * student_gain.astype(F32)).astype(BF16)
    depth = w_gate.shape[0]

    def part(arr, owner, width):
        return lax.dynamic_slice_in_dim(arr, owner * width, width, 1)

    def add_rows(blocks):
        total = None
        for owner, block in zip(owners, blocks):
            piece = jnp.dot(part(normed, owner, depth), block, preferred_element_type=F32)
            total = piece if total is None else total + piece
        return total

    gate_acts = add_rows(gates)
    up_acts = add_rows(ups)
    hidden = (jax.nn.silu(gate_acts) * up_acts).astype(BF16)

    width = w_down.shape[1]
    outs = []
    for s in range(n_x):
        pair = [
            jnp.dot(hidden, downs[s * cores + f], preferred_element_type=F32).astype(BF16)
            for f in range(cores)
        ]
        sums = lax.psum(jnp.concatenate(pair, axis=1), "tensor")
        for f in range(cores):
            here = part(x_bf, owners[s * cores + f], width).astype(F32)
            mlp = sums[:, f * width : (f + 1) * width].astype(F32)
            outs.append((here + mlp).astype(BF16))

    target = None
    for owner, block in zip(owners, finals):
        dest = lax.dynamic_slice_in_dim(dest_row, owner * tile_rows, tile_rows, 0)
        mine = dp_at * tile_rows + jnp.arange(tile_rows)
        pick = (mine[:, None] == dest[None, :]).astype(BF16)
        piece = jnp.dot(pick, block, preferred_element_type=F32)
        target = piece if target is None else target + piece

    residue = -target
    for block, rows in zip(outs, projs):
        residue = residue + jnp.dot(block, rows, preferred_element_type=F32)
    row_loss = lax.psum(jnp.sum(residue * residue, axis=1), "tensor") / ht

    local_cols = student_in.shape[1]
    start = tensor_at * local_cols
    owner = start // width
    place = ((owner // cores - x_at) % n_x) * cores + (owner % cores - core_at) % cores
    inner = start % width
    out_local = lax.dynamic_slice_in_dim(
        jnp.concatenate(outs, axis=1), place * width + inner, local_cols, 1
    )
    return (out_local, row_loss, residue)


def solution(mesh):
    placed = (
        P("dp", "tensor"),
        P("tensor", None),
        P(("dp", "tensor"), None),
        P(),
        P(),
        P("dp", "tensor"),
        P(),
        P("dp", "tensor"),
        P("dp", "tensor"),
        P("tensor", "dp"),
        P("dp", "tensor"),
    )
    return jax.shard_map(
        local,
        mesh=mesh,
        in_specs=placed,
        out_specs=(P("dp", "tensor"), P("dp"), P("dp", "tensor")),
        check_vma=False,
    )
```
